512 devices in a mesh: seq: 64 (over x, z), tensor: 8 (over y, core).
Axes of the slice: x: 4, y: 4, z: 16, core: 2. Of those that a mesh axis runs over, the one named last changes fastest.
Arguments:
- hidden: bfloat16 [8, 16384, 8192], P(None, 'seq', 'tensor'), may hold values from -160 to 160
- norm_gain: bfloat16 [8192], P('tensor'), may hold values from 0.25 to 1.75
- value_weight: bfloat16 [8192], P('tensor'), may hold values from -0.0625 to 0.0625
- rewards: float32 [8, 16384], P(None, 'seq'), may hold values from -6 to 6
- done_flags: int32 [8, 16384], P(None, 'seq'), may hold values 0 or 1
- valid_mask: int32 [8, 16384], P('tensor', 'seq'), may hold values 0 or 1
- new_logprob: float32 [8, 16384], P('tensor', 'seq'), may hold values from -1 to 1
- old_logprob: float32 [8, 16384], P('tensor', 'seq'), may hold values from -1 to 1
- discount: float32 [8], replicated, may hold values from 0.9 to 1
- trace_decay: float32 [8], replicated, may hold values from 0.9 to 1
- bootstrap: float32 [8], replicated, may hold values from -5 to 5
Outputs:
- values: float32 [8, 16384], P('tensor', 'seq')
- white_adv: float32 [8, 16384], P('tensor', 'seq')
- token_loss: float32 [8, 16384], P('tensor', 'seq')
- policy_loss: float32 [], replicated
The draws below stay inside these ranges and needn't reach their ends.
All inputs are finite; a program needn't handle non-finite values. No bound on the sum of `done_flags` or of `valid_mask` on one device may be relied on, other than what follows from the above.
Results may differ from the reference program's by a relative error of at most 0.00035.
Values sent between devices are 32-bit elements; how exact they have to be, the bound alone decides.
A program may use at most 64 MiB of HBM per device.

```python
import math
from functools import partial
import jax
import jax.numpy as jnp
from jax import lax

H = 8192
LEN_DEV = 256
SEQS = 8
LENGTH = 16384


def draw_hidden(key, part):
    k_base, k_cols = jax.random.split(jax.random.fold_in(key, 11), 2)
    base = jax.random.truncated_normal(k_base, -4.0, 4.0, (SEQS, LENGTH, H), jnp.float32)
    columns = jnp.exp(jax.random.uniform(k_cols, (H,), jnp.float32) * math.log(10.0))
    drawn = base * columns
    return drawn.astype(jnp.bfloat16)


def draw_discount(key, part):
    k_main = jax.random.fold_in(key, 23)
    spread = jax.random.uniform(k_main, (SEQS,), jnp.float32, 0.1, 0.5)
    return 1.0 - spread / LENGTH


def draw_trace_decay(key, part):
    k_pick, k_slow, k_fast = jax.random.split(jax.random.fold_in(key, 37), 3)
    quick = jax.random.bernoulli(k_pick, 0.5, (SEQS,))
    slow_rate = 1.0 - jax.random.uniform(k_slow, (SEQS,), jnp.float32, 0.2, 1.0) / LENGTH
    fast_rate = 1.0 - jax.random.uniform(k_fast, (SEQS,), jnp.float32, 0.02, 0.033)
    return jnp.where(quick, fast_rate, slow_rate)


def touch_ends(entries, stream_key, low, largest):
    index_at = [jax.random.randint(jax.random.fold_in(stream_key, axis), (), 0, length) for axis, length in enumerate(entries.shape)]
    longest = entries.shape.index(max(entries.shape))
    beside = index_at[:longest] + [(index_at[longest] + 1) % entries.shape[longest]] + index_at[longest + 1:]
    return entries.at[tuple(index_at)].set(low).at[tuple(beside)].set(largest)


def block_scale(own_key, extent, shards, smallest, high):
    factor_of = 1.0
    for position, parts in shards:
        steps = jax.random.uniform(jax.random.fold_in(jax.random.fold_in(own_key, 6), position), (parts,), jnp.float32, smallest / len(shards), high / len(shards))
        factor_of = factor_of * jnp.repeat(jnp.exp(steps), extent[position] // parts).reshape((-1,) + (1,) * (len(extent) - 1 - position))
    return factor_of


def noise(key, dims, deviation, limit, shards=(), held_as=jnp.bfloat16):
    values = deviation * jax.random.normal(key, dims, jnp.float32)
    if shards:
        values = values * block_scale(key, dims, shards, -0.22, 0.18)
    return jnp.clip(values, -limit, limit).astype(held_as)


def setup_inputs(seed: int = 0) -> dict:
    seeds = jax.random.split(jax.random.key(seed), 12)
    return {
        "hidden": draw_hidden(jax.random.fold_in(seeds[11], 71), 0),
        "norm_gain": jnp.clip(1.0 + 0.15 * jax.random.normal(seeds[1], (H,), jnp.float32), 0.25, 1.75).astype(jnp.bfloat16),
        "value_weight": noise(seeds[2], (H,), H ** -0.5, 0.0625, ((0, 8),)),
        "rewards": noise(seeds[3], (SEQS, LENGTH), 1.0, 6.0, ((1, 64),), jnp.float32),
        "done_flags": touch_ends((jax.random.randint(seeds[4], (SEQS, LENGTH), 0, 128 * LEN_DEV) < 1).astype(jnp.int32), jax.random.fold_in(seeds[4], 1), 0, 1),
        "valid_mask": touch_ends((jax.random.randint(seeds[5], (SEQS, LENGTH), 0, 4) < 3).astype(jnp.int32), jax.random.fold_in(seeds[5], 1), 0, 1),
        "new_logprob": noise(seeds[6], (SEQS, LENGTH), 0.15, 1.0, ((0, 8), (1, 64)), jnp.float32),
        "old_logprob": noise(seeds[7], (SEQS, LENGTH), 0.15, 1.0, ((0, 8), (1, 64)), jnp.float32),
        "discount": draw_discount(jax.random.fold_in(seeds[11], 71), 0),
        "trace_decay": draw_trace_decay(jax.random.fold_in(seeds[11], 71), 0),
        "bootstrap": noise(seeds[10], (SEQS,), 1.0, 5.0, (), jnp.float32),
    }


EPS_NORM = 1e-06
EPS_WHITE = 1e-08
CLIP = 0.2

def head_block(scaled, block):
    wide = block.astype(jnp.float32)
    squares = lax.optimization_barrier(jnp.sum(wide * wide, axis=-1))
    products = jnp.dot(wide, scaled, precision=lax.Precision.HIGHEST)
    return products * lax.rsqrt(squares / H + EPS_NORM)

def backward_step(carry, inputs):
    delta_now, coef_now = inputs
    fresh = delta_now + coef_now * carry
    return (fresh, fresh)

def reference(hidden, norm_gain, value_weight, rewards, done_flags, valid_mask, new_logprob, old_logprob, discount, trace_decay, bootstrap):
    scaled = norm_gain.astype(jnp.float32) * value_weight.astype(jnp.float32)
    blocks = hidden.reshape(SEQS * LENGTH // LEN_DEV, LEN_DEV, H)
    values = lax.map(partial(head_block, scaled), blocks).reshape(SEQS, LENGTH)
    alive = 1.0 - done_flags.astype(jnp.float32)
    following = jnp.concatenate([values[:, 1:], bootstrap[:, None]], axis=1)
    delta = rewards + discount[:, None] * alive * following - values
    decay = discount * trace_decay
    coefs = decay[:, None] * alive
    start = jnp.zeros((SEQS,), jnp.float32)
    _, stacked = lax.scan(backward_step, start, (delta.T, coefs.T), reverse=True)
    advantages = stacked.T
    weight = valid_mask.astype(jnp.float32)
    count = jnp.sum(weight)
    mean = jnp.sum(weight * advantages) / count
    variance = jnp.sum(weight * (advantages - mean) ** 2) / count
    white_adv = (advantages - mean) * lax.rsqrt(variance + EPS_WHITE)
    ratio = jnp.exp(new_logprob - old_logprob)
    surrogate = jnp.minimum(ratio * white_adv, jnp.clip(ratio, 1.0 - CLIP, 1.0 + CLIP) * white_adv)
    token_loss = -weight * surrogate
    policy_loss = jnp.sum(token_loss) / count
    return (values, white_adv, token_loss, policy_loss)
```

```python
from functools import partial

import jax
import jax.numpy as jnp
from jax import lax
from jax.experimental import pallas as pl
from jax.experimental.pallas import tpu as pltpu
from jax.sharding import PartitionSpec as P

EPS_NORM = 1e-06
EPS_WHITE = 1e-08
CLIP = 0.2
LANES = 128
SUBS = 8
EXTRA = 16
F32 = jnp.float32
MESH = pl.DeviceIdType.MESH


def chip_grid(seq_count):
    return {64: (4, 16), 16: (4, 4), 4: (2, 2)}[seq_count]


def offsets_by_distance(nx, ny):
    def far(o):
        return min(o[0], nx - o[0]) + min(o[1], ny - o[1])

    every = [(dx, dy, dc) for dx in range(nx) for dy in range(ny) for dc in range(2)]
    return sorted(every[1:], key=lambda o: (-far(o), -o[2]))


def shift_lanes(x, count, fill, lane, width):
    moved = pltpu.roll(x, width - count, 1)
    return jnp.where(lane >= width - count, fill, moved)


def shift_rows(x, count, fill, row, height):
    moved = pltpu.roll(x, height - count, 0)
    return jnp.where(row >= height - count, fill, moved)


def picked(table, index):
    return jnp.take_along_axis(table, jnp.full(table.shape, index, jnp.int32), axis=1)


def kernel(
    sizes,
    hid, gain, wgt, rew, done, mask, newp, oldp, disc, trace, boot,
    out_v, out_w, out_l, out_s,
    buf, gain_v, wgt_v, rew_v, done_v, mask_v, new_v, old_v, disc_s, trace_s, boot_s,
    send_a, recv_a, mess_b, recv_b, mess_c, recv_c, mess_d, recv_d, mess_e, recv_e,
    res_v, res_w, res_l, res_s,
    hid_sem, in_sem, send_sem, recv_sem, out_sem,
):
    nx, nz, ny, length, features, total_features = sizes
    rows = 2 * ny
    seq = lax.axis_index("seq")
    t = lax.axis_index("tensor")
    x, z = lax.div(seq, nz), lax.rem(seq, nz)
    y, core = lax.div(t, 2), lax.rem(t, 2)

    def plane_peer(o):
        px = lax.rem(x + o[0], nx)
        py = lax.rem(y + o[1], ny)
        pc = core if o[2] == 0 else 1 - core
        return px, py * 2 + pc

    def ring_peer(d):
        return {"seq": x * nz + lax.rem(z + d, nz), "tensor": t}

    plane = offsets_by_distance(nx, ny)
    column = [o for o in plane if o[0] == 0] + [(0, 0, 0)]
    ring = sorted(range(1, nz), key=lambda d: -min(d, nz - d))

    order = [plane_peer(o)[1] for o in column]
    loads = [
        pltpu.make_async_copy(hid.at[order[k]], buf.at[k, pl.ds(0, length)], hid_sem.at[k])
        for k in range(rows)
    ]
    small = [
        (gain, gain_v), (wgt, wgt_v), (rew, rew_v), (done, done_v), (mask, mask_v),
        (newp, new_v), (oldp, old_v), (disc, disc_s), (trace, trace_s), (boot, boot_s),
    ]
    small = [pltpu.make_async_copy(a, b, in_sem.at[i]) for i, (a, b) in enumerate(small)]
    for c in small[:2]:
        c.start()
    for c in loads:
        c.start()
    for c in small[2:]:
        c.start()

    barrier = pltpu.get_barrier_semaphore()
    for d in ring:
        pl.semaphore_signal(barrier, inc=1, device_id=ring_peer(d), device_id_type=MESH)
    for o in plane:
        px, pt = plane_peer(o)
        pl.semaphore_signal(
            barrier, inc=1, device_id={"seq": px * nz + z, "tensor": pt}, device_id_type=MESH
        )

    for c in small[:2]:
        c.wait()
    scaled = gain_v[...].astype(F32) * wgt_v[...].astype(F32)
    high = scaled.astype(jnp.bfloat16).astype(F32)
    low = scaled - high
    extra_row = lax.broadcasted_iota(jnp.int32, (EXTRA, features), 0)
    both = jnp.where(
        extra_row == 0,
        jnp.broadcast_to(high.reshape(1, features), (EXTRA, features)),
        jnp.where(extra_row == 1, jnp.broadcast_to(low.reshape(1, features), (EXTRA, features)), 0.0),
    ).astype(jnp.bfloat16)
    for k in range(rows):
        buf[k, pl.ds(length, EXTRA)] = both

    eye = lax.broadcasted_iota(jnp.int32, (length, length), 0) == lax.broadcasted_iota(
        jnp.int32, (length, length), 1
    )
    for k in range(rows):
        loads[k].wait()
        gram = lax.dot_general(
            buf[k], buf[k, pl.ds(0, length)], (((1,), (1,)), ((), ())), preferred_element_type=F32
        )
        squares = jnp.sum(jnp.where(eye, gram[:length], 0.0), axis=0, keepdims=True)
        products = gram[length : length + 1] + gram[length + 1 : length + 2]
        if k < rows - 1:
            send_a[k, :, pl.ds(0, length)] = squares
            send_a[k, :, pl.ds(length, length)] = products
        else:
            recv_a[t, :, pl.ds(0, length)] = squares
            recv_a[t, :, pl.ds(length, length)] = products

    pl.semaphore_wait(barrier, nz - 1 + nx * rows - 1)

    def push(src, dst, stage, device):
        copy = pltpu.make_async_remote_copy(
            src_ref=src, dst_ref=dst, send_sem=send_sem.at[stage], recv_sem=recv_sem.at[stage],
            device_id=device, device_id_type=MESH,
        )
        copy.start()

    def arrived(slots, count, stage):
        part = slots.at[pl.ds(0, count)]
        pltpu.make_async_copy(part, part, recv_sem.at[stage]).wait()

    def left(slots, count, stage):
        part = slots.at[pl.ds(0, count)]
        pltpu.make_async_copy(part, part, send_sem.at[stage]).wait()

    def to_ring(mess, slots, stage):
        for d in ring:
            push(mess, slots.at[z], stage, ring_peer(d))

    def to_plane(mess, slots, stage):
        for o in plane:
            px, pt = plane_peer(o)
            push(mess, slots.at[x * rows + t], stage, {"seq": px * nz + z, "tensor": pt})

    for k in range(rows - 1):
        push(send_a.at[k], recv_a.at[t], 0, {"seq": seq, "tensor": order[k]})

    for c in small[2:]:
        c.wait()
    gamma, lam = disc_s[t], trace_s[t]
    wide = (SUBS, length)
    lane = lax.broadcasted_iota(jnp.int32, wide, 1)
    sub = lax.broadcasted_iota(jnp.int32, wide, 0)

    def spread(a):
        return jnp.broadcast_to(a, wide)

    rewards = spread(rew_v[pl.ds(t, 1)])
    alive = 1.0 - spread(done_v[pl.ds(t, 1)]).astype(F32)
    weight = spread(mask_v[...]).astype(F32)
    ratio = jnp.exp(spread(new_v[...]) - spread(old_v[...]))
    clipped = jnp.clip(ratio, 1.0 - CLIP, 1.0 + CLIP)
    last_pos = lane == length - 1
    reach = gamma * alive
    coef = jnp.where(last_pos, reach, (gamma * lam) * alive)
    coefs = []
    for step in range(length.bit_length() - 1):
        coefs.append(coef)
        coef = coef * shift_lanes(coef, 1 << step, 1.0, lane, length)
    ends = jnp.logical_and(x == nx - 1, z == nz - 1)
    known = jnp.where(ends, boot_s[t], 0.0)
    kept = jnp.where(ends, 0.0, 1.0)
    n_own = jnp.sum(weight, axis=1, keepdims=True)
    n_inv = 1.0 / jnp.maximum(n_own, 1.0)

    arrived(recv_a, rows - 1, 0)
    sums = jnp.sum(recv_a[...], axis=0)
    values = spread(sums[:, length:] * lax.rsqrt(sums[:, :length] / total_features + EPS_NORM))
    res_v[...] = values[:1]
    v_copy = pltpu.make_async_copy(res_v, out_v, out_sem.at[0])
    v_copy.start()

    local = rewards + reach * shift_lanes(values, 1, 0.0, lane, length) - values
    for step, c in enumerate(coefs):
        local = local + c * shift_lanes(local, 1 << step, 0.0, lane, length)
    local = local + coef * known
    coef = coef * kept
    mean_l = jnp.sum(weight * local, axis=1, keepdims=True) * n_inv
    mean_c = jnp.sum(weight * coef, axis=1, keepdims=True) * n_inv
    dev_l, dev_c = local - mean_l, coef - mean_c
    w_l, w_c = weight * dev_l, weight * dev_c
    table = jnp.zeros(wide, F32)
    first = lane == 0
    for i, q in enumerate(
        [jnp.where(first, values + lam * local, 0.0), jnp.where(first, lam * coef, 0.0),
         w_l * dev_l, w_l * dev_c, w_c * dev_c]
    ):
        table = jnp.where(sub == i, q, table)
    column_of = jnp.sum(table, axis=1, keepdims=True)
    sub1 = lax.broadcasted_iota(jnp.int32, (SUBS, 1), 0)
    for i, q in [(5, n_own), (6, mean_l), (7, mean_c)]:
        column_of = jnp.where(sub1 == i, q, column_of)
    tile = (SUBS, LANES)
    on_diagonal = lax.broadcasted_iota(jnp.int32, tile, 0) == lax.broadcasted_iota(jnp.int32, tile, 1)
    message = jnp.sum(
        jnp.where(on_diagonal, jnp.broadcast_to(column_of, tile), 0.0), axis=0, keepdims=True
    )
    mess_b[...] = message
    recv_b[z] = message
    to_ring(mess_b, recv_b, 1)

    arrived(recv_b, nz - 1, 1)
    got = recv_b[:, 0, :]
    row = lax.broadcasted_iota(jnp.int32, (nz, LANES), 0)
    zlane = lax.broadcasted_iota(jnp.int32, (nz, LANES), 1)
    o, s, m_ll, m_lc, m_cc, n, mu_l, mu_c = (picked(got, i) for i in range(8))
    run_o, run_s, step = o, s, 1
    while step < nz:
        run_o = run_o + run_s * shift_rows(run_o, step, 0.0, row, nz)
        run_s = run_s * shift_rows(run_s, step, 1.0, row, nz)
        step *= 2
    p = shift_rows(run_o, 1, 0.0, row, nz)
    q = shift_rows(run_s, 1, 1.0, row, nz)

    def down(a):
        return jnp.sum(a, axis=0, keepdims=True)

    a_blk, b_blk = mu_l + mu_c * p, mu_c * q
    n_line = down(n)
    n_line_inv = 1.0 / jnp.maximum(n_line, 1.0)
    a_line, b_line = down(n * a_blk) * n_line_inv, down(n * b_blk) * n_line_inv
    da, db = a_blk - a_line, b_blk - b_line
    m_aa = m_ll + 2.0 * p * m_lc + p * p * m_cc + n * da * da
    m_ab = q * m_lc + p * q * m_cc + n * da * db
    m_bb = q * q * m_cc + n * db * db
    line = jnp.where(zlane == 2, m_aa, jnp.where(zlane == 3, m_ab, jnp.where(zlane == 4, m_bb, 0.0)))
    line = jnp.where(
        row == 0, jnp.where(zlane == 0, run_o, jnp.where(zlane == 1, run_s, line)), line
    )
    message = down(line)
    lane1 = lax.broadcasted_iota(jnp.int32, (1, LANES), 1)
    for i, v in [(5, n_line), (6, a_line), (7, b_line)]:
        message = jnp.where(lane1 == i, v, message)
    mess_c[...] = message
    recv_c[x * rows + t] = message
    to_plane(mess_c, recv_c, 2)
    own_p = down(jnp.where(row == z, p, 0.0))
    own_q = down(jnp.where(row == z, q, 0.0))

    arrived(recv_c, nx * rows - 1, 2)
    got = recv_c[:, 0, :].reshape(nx, rows, LANES)
    rsub = lax.broadcasted_iota(jnp.int32, (rows, LANES), 0)
    entering = jnp.zeros((rows, LANES), F32)
    own_e = jnp.zeros((rows, LANES), F32)
    lines = []
    for i in reversed(range(nx)):
        o, s, m_aa, m_ab, m_bb, n, a, b = (picked(got[i], j) for j in range(8))
        own_e = jnp.where(jnp.logical_and(rsub == t, x == i), entering, own_e)
        lines.append(
            (n, a + b * entering, m_aa + 2.0 * entering * m_ab + entering * entering * m_bb)
        )
        entering = o + s * entering
    count = down(sum(n for n, _, _ in lines))
    mean = down(sum(n * mu for n, mu, _ in lines)) / count
    second = down(sum(m + n * (mu - mean) * (mu - mean) for n, mu, m in lines))
    scale = lax.rsqrt(second / count + EPS_WHITE)
    enter = own_p + own_q * down(own_e)

    def over(a):
        return jnp.broadcast_to(jnp.concatenate([a] * (length // LANES), axis=1), wide)

    white = (local + coef * over(enter) - over(mean)) * over(scale)
    loss = -weight * jnp.minimum(ratio * white, clipped * white)
    message = jnp.broadcast_to(jnp.sum(loss, axis=1, keepdims=True), tile)[:1]
    mess_d[...] = message
    recv_d[z] = message
    to_ring(mess_d, recv_d, 3)
    res_w[...] = white[:1]
    res_l[...] = loss[:1]
    w_copy = pltpu.make_async_copy(res_w, out_w, out_sem.at[1])
    w_copy.start()
    l_copy = pltpu.make_async_copy(res_l, out_l, out_sem.at[2])
    l_copy.start()

    arrived(recv_d, nz - 1, 3)
    message = down(recv_d[:, 0, :])
    mess_e[...] = message
    recv_e[x * rows + t] = message
    to_plane(mess_e, recv_e, 4)
    arrived(recv_e, nx * rows - 1, 4)
    res_s[...] = down(recv_e[:, 0, :]) / count
    s_copy = pltpu.make_async_copy(res_s, out_s, out_sem.at[3])
    s_copy.start()

    left(recv_a, rows - 1, 0)
    left(recv_b, nz - 1, 1)
    left(recv_c, nx * rows - 1, 2)
    left(recv_d, nz - 1, 3)
    left(recv_e, nx * rows - 1, 4)
    for c in (v_copy, w_copy, l_copy, s_copy):
        c.wait()


def shards(seq_count, total_features, *args):
    hidden = args[0]
    rows, length, features = hidden.shape
    nx, nz = chip_grid(seq_count)
    ny = rows // 2
    any_space = pl.BlockSpec(memory_space=pl.ANY)
    vmem, smem = pltpu.VMEM, pltpu.SMEM
    out = jax.ShapeDtypeStruct((1, length), F32)
    values, white, loss, total = pl.pallas_call(
        partial(kernel, (nx, nz, ny, length, features, total_features)),
        out_shape=[out, out, out, jax.ShapeDtypeStruct((1, LANES), F32)],
        in_specs=[any_space] * 11,
        out_specs=[any_space] * 4,
        scratch_shapes=[
            vmem((rows, length + EXTRA, features), jnp.bfloat16),
            vmem((features,), jnp.bfloat16),
            vmem((features,), jnp.bfloat16),
            vmem((rows, length), F32),
            vmem((rows, length), jnp.int32),
            vmem((1, length), jnp.int32),
            vmem((1, length), F32),
            vmem((1, length), F32),
            smem((rows,), F32),
            smem((rows,), F32),
            smem((rows,), F32),
            vmem((rows, 1, 2 * length), F32),
            vmem((rows, 1, 2 * length), F32),
            vmem((1, LANES), F32),
            vmem((nz, 1, LANES), F32),
            vmem((1, LANES), F32),
            vmem((nx * rows, 1, LANES), F32),
            vmem((1, LANES), F32),
            vmem((nz, 1, LANES), F32),
            vmem((1, LANES), F32),
            vmem((nx * rows, 1, LANES), F32),
            vmem((1, length), F32),
            vmem((1, length), F32),
            vmem((1, length), F32),
            vmem((1, LANES), F32),
            pltpu.SemaphoreType.DMA((rows,)),
            pltpu.SemaphoreType.DMA((10,)),
            pltpu.SemaphoreType.DMA((5,)),
            pltpu.SemaphoreType.DMA((5,)),
            pltpu.SemaphoreType.DMA((4,)),
        ],
        compiler_params=pltpu.CompilerParams(collective_id=0, has_side_effects=True),
        name="critic_gae",
    )(*args)
    return values, white, loss, total[0, 0]


def solution(mesh):
    seq_only = P(None, "seq")
    both = P("tensor", "seq")
    in_specs = (
        P(None, "seq", "tensor"), P("tensor"), P("tensor"), seq_only, seq_only,
        both, both, both, P(), P(), P(),
    )
    total_features = 1024 * mesh.shape["tensor"]
    return jax.shard_map(
        partial(shards, mesh.shape["seq"], total_features),
        mesh=mesh, in_specs=in_specs, out_specs=(both, both, both, P()), check_vma=False,
    )
```
